8 devices in a mesh: fsdp: 2 (over z, y), ep: 4 (over x, core).
Axes of the slice: x: 2, y: 2, z: 1, core: 2. Of those that a mesh axis runs over, the one named last changes fastest.
Arguments:
- grad_out: bfloat16 [16384, 768], P(('fsdp', 'ep'))
- expert_idx: int32 [16384, 1], P(('fsdp', 'ep'))
- slot_pos: int32 [16384, 1], P(('fsdp', 'ep'))
- gates: float32 [16384, 1], P(('fsdp', 'ep'))
- x_disp: bfloat16 [8, 2560, 768], P('ep', 'fsdp')
- h_gate: bfloat16 [8, 2560, 3072], P('ep', 'fsdp')
- h_up: bfloat16 [8, 2560, 3072], P('ep', 'fsdp')
- y_disp: bfloat16 [8, 2560, 768], P('ep', 'fsdp')
- w_gate: bfloat16 [8, 768, 3072], P('ep', 'fsdp')
- w_down: bfloat16 [8, 3072, 768], P('ep', 'fsdp')
- w_up: bfloat16 [8, 768, 3072], P('ep', 'fsdp')
Outputs:
- output 1: bfloat16 [16384, 768], P(('fsdp', 'ep'))
- output 2: float32 [16384, 1], P(('fsdp', 'ep'))
- output 3: float32 [8, 768, 3072], P('ep', 'fsdp')
- output 4: float32 [8, 3072, 768], P('ep', 'fsdp')
- output 5: float32 [8, 768, 3072], P('ep', 'fsdp')
All inputs are finite; a program needn't handle non-finite values.
Results may differ from the reference program's by a relative error of at most 0.001.
Values are sent between devices in bfloat16 or wider.
A program may use at most 1 GiB of HBM per device.

```python
import jax
import jax.numpy as jnp
from jax import lax

D = 768
F = 3072
EXPERTS = 8
TOP = 1
TOK = 2048
NDEV = 8
CAP = 320


def route_draw(key):
    key_bias, key_noise, key_hot = jax.random.split(key, 3)
    expert_ids = jnp.arange(EXPERTS, dtype=jnp.int32)
    expert_bias = jax.random.randint(key_bias, (EXPERTS,), 0, 512, dtype=jnp.int32)
    noise_int = jax.random.randint(key_noise, (NDEV, TOK, EXPERTS), 0, 1024, dtype=jnp.int32)
    hot_expert = jax.random.randint(key_hot, (NDEV,), 0, EXPERTS, dtype=jnp.int32)
    forced = (jnp.arange(TOK, dtype=jnp.int32)[None, :, None] <= CAP) & (expert_ids[None, None, :] == hot_expert[:, None, None])
    score_int = (noise_int + expert_bias + jnp.where(forced, 4096, 0)) * EXPERTS + expert_ids
    expert_idx = lax.top_k(score_int, TOP)[1].astype(jnp.int32)

    def block_slots(block_idx):
        flat_ids = block_idx.reshape(-1)
        hit_mask = (flat_ids[:, None] == expert_ids[None, :]).astype(jnp.int32)
        slot_rank = jnp.sum((jnp.cumsum(hit_mask, axis=0) - hit_mask) * hit_mask, axis=1)
        return jnp.where(slot_rank < CAP, slot_rank, -1).reshape(TOK, TOP)

    slot_pos = lax.map(block_slots, expert_idx)
    return expert_idx.reshape(NDEV * TOK, TOP), slot_pos.reshape(NDEV * TOK, TOP).astype(jnp.int32)


def setup_inputs(seed: int = 0) -> dict:
    keys = jax.random.split(jax.random.key(seed), 11)
    expert_idx, slot_pos = route_draw(keys[0])
    rows_all = NDEV * CAP
    grad_out = jax.random.normal(keys[1], (NDEV * TOK, D), jnp.float32).astype(jnp.bfloat16)
    gates = jax.random.uniform(keys[2], (NDEV * TOK, TOP), jnp.float32, 0.2, 1.0)
    x_disp = jax.random.normal(keys[3], (EXPERTS, rows_all, D), jnp.float32).astype(jnp.bfloat16)
    h_gate = jax.random.normal(keys[4], (EXPERTS, rows_all, F), jnp.float32).astype(jnp.bfloat16)
    h_up = jax.random.normal(keys[5], (EXPERTS, rows_all, F), jnp.float32).astype(jnp.bfloat16)
    y_disp = (0.25 * jax.random.normal(keys[6], (EXPERTS, rows_all, D), jnp.float32)).astype(jnp.bfloat16)
    w_gate = (jax.random.normal(keys[7], (EXPERTS, D, F), jnp.float32) * D ** -0.5).astype(jnp.bfloat16)
    w_down = (jax.random.normal(keys[8], (EXPERTS, F, D), jnp.float32) * F ** -0.5).astype(jnp.bfloat16)
    w_up = (jax.random.normal(keys[9], (EXPERTS, D, F), jnp.float32) * D ** -0.5).astype(jnp.bfloat16)
    return {'grad_out': grad_out, 'expert_idx': expert_idx, 'slot_pos': slot_pos, 'gates': gates, 'x_disp': x_disp, 'h_gate': h_gate, 'h_up': h_up, 'y_disp': y_disp, 'w_gate': w_gate, 'w_down': w_down, 'w_up': w_up}


def expert_backward(operands):
    dy_rows, gate_rows, x_rows, pre_gate, pre_up, y_rows, w_gate, w_down, w_up = operands
    g_rows = (dy_rows.astype(jnp.float32) * gate_rows[:, None]).astype(jnp.bfloat16)
    gate_pre = pre_gate.astype(jnp.float32)
    up_pre = pre_up.astype(jnp.float32)
    sigmoid_gate = jax.nn.sigmoid(gate_pre)
    silu_gate = gate_pre * sigmoid_gate
    act_rows = (silu_gate * up_pre).astype(jnp.bfloat16)
    d_act = jnp.dot(g_rows, w_down.T, preferred_element_type=jnp.float32)
    dh_gate = (d_act * up_pre * sigmoid_gate * (1.0 + gate_pre * (1.0 - sigmoid_gate))).astype(jnp.bfloat16)
    dh_up = (d_act * silu_gate).astype(jnp.bfloat16)
    dx_rows = (jnp.dot(dh_gate, w_gate.T, preferred_element_type=jnp.float32) + jnp.dot(dh_up, w_up.T, preferred_element_type=jnp.float32)).astype(jnp.bfloat16)
    dgate_rows = jnp.sum(dy_rows.astype(jnp.float32) * y_rows.astype(jnp.float32), axis=1)
    dw_gate = jnp.dot(x_rows.T, dh_gate, preferred_element_type=jnp.float32)
    dw_down = jnp.dot(act_rows.T, g_rows, preferred_element_type=jnp.float32)
    dw_up = jnp.dot(x_rows.T, dh_up, preferred_element_type=jnp.float32)
    return dx_rows, dgate_rows, dw_gate, dw_down, dw_up


def reference(grad_out, expert_idx, slot_pos, gates, x_disp, h_gate, h_up, y_disp, w_gate, w_down, w_up):
    rows_all = NDEV * CAP
    choices = NDEV * TOK * TOP
    block_ids = jnp.arange(NDEV * TOK, dtype=jnp.int32)[:, None] // TOK
    dest_row = jnp.where(slot_pos >= 0, expert_idx * rows_all + block_ids * CAP + slot_pos, EXPERTS * rows_all).reshape(-1)
    src_choice = jnp.full((EXPERTS * rows_all,), choices, jnp.int32).at[dest_row].set(jnp.arange(choices, dtype=jnp.int32), mode='drop')
    dy_rows = jnp.take(grad_out, src_choice // TOP, axis=0, mode='fill', fill_value=0).reshape(EXPERTS, rows_all, D)
    gate_rows = jnp.take(gates.reshape(-1), src_choice, mode='fill', fill_value=0).reshape(EXPERTS, rows_all)
    dx_rows, dgate_rows, dw_gate, dw_down, dw_up = lax.map(expert_backward, (dy_rows, gate_rows, x_disp, h_gate, h_up, y_disp, w_gate, w_down, w_up))
    picked = jnp.take(dx_rows.reshape(EXPERTS * rows_all, D), dest_row, axis=0, mode='fill', fill_value=0).reshape(NDEV * TOK, TOP, D)
    grad_x = jnp.sum(picked.astype(jnp.float32), axis=1).astype(jnp.bfloat16)
    grad_gates = jnp.take(dgate_rows.reshape(-1), dest_row, mode='fill', fill_value=0).reshape(NDEV * TOK, TOP)
    return grad_x, grad_gates, dw_gate, dw_down, dw_up
```

```python
import jax
import jax.numpy as jnp
from jax import lax
from jax.sharding import PartitionSpec as P

CHUNK = 256


def solution(mesh):
    ep_n = mesh.shape['ep']
    fs_n = mesh.shape['fsdp']
    tok_spec = P(('fsdp', 'ep'), None)
    row_spec = P('ep', 'fsdp', None)
    swap = [(0, 1), (1, 0)]

    def local_backward(grad_out, expert_idx, slot_pos, gates, x_disp, h_gate, h_up, y_disp, w_gate, w_down, w_up):
        f32, bf16 = jnp.float32, jnp.bfloat16
        tok_n = expert_idx.shape[0]
        e_loc, rows_loc, width = x_disp.shape
        hid = h_gate.shape[2]
        w_half, h_half = width // fs_n, hid // fs_n
        slot_cap = rows_loc // ep_n
        slots_n = e_loc * ep_n * slot_cap
        me_q = lax.axis_index('fsdp')
        me_p = lax.axis_index('ep')

        full_w_down = lax.all_gather(w_down, 'fsdp', axis=1, tiled=True)

        ids = expert_idx[:, 0]
        slots = slot_pos[:, 0]
        hits = (ids[:, None] == jnp.arange(e_loc * ep_n, dtype=jnp.int32)[None, :]) & (slots >= 0)[:, None]
        counts = lax.all_gather(jnp.sum(hits.astype(jnp.int32), axis=0), ('fsdp', 'ep'), axis=0)
        counts = lax.dynamic_slice(counts.reshape(fs_n, ep_n, ep_n, e_loc), (0, 0, me_p, 0), (fs_n, ep_n, 1, e_loc))[:, :, 0, :]
        totals = jnp.sum(counts, axis=1)
        mine = lax.dynamic_index_in_dim(counts, me_q, 0, keepdims=False)
        starts = jnp.cumsum(mine, axis=0) - mine
        filled = lax.dynamic_index_in_dim(totals, me_q, 0, keepdims=False)
        filled_peer = lax.dynamic_index_in_dim(totals, 1 - me_q, 0, keepdims=False)
        chunks = jnp.maximum((jnp.max(totals, axis=0) + CHUNK - 1) // CHUNK, 1)

        send_row = jnp.where(slots >= 0, ((ids % e_loc) * ep_n + ids // e_loc) * slot_cap + slots, slots_n)
        src_choice = jnp.full((slots_n,), tok_n, jnp.int32).at[send_row].set(jnp.arange(tok_n, dtype=jnp.int32), mode='drop')
        send_dy = jnp.take(grad_out, src_choice, axis=0, mode='fill', fill_value=0).reshape(e_loc, ep_n, slot_cap, width)
        send_gate = jnp.take(gates.reshape(-1), src_choice, mode='fill', fill_value=0).reshape(e_loc, ep_n, slot_cap)
        recv_dy = lax.all_to_all(send_dy, 'ep', 1, 1, tiled=True).reshape(e_loc, rows_loc, width)
        recv_gate = lax.all_to_all(send_gate, 'ep', 1, 1, tiled=True).reshape(e_loc, rows_loc)
        dgate_rows = jnp.sum(recv_dy.astype(f32) * y_disp.astype(f32), axis=2)
        back_gate = lax.all_to_all(dgate_rows.reshape(e_loc, ep_n, slot_cap), 'ep', 1, 1, tiled=True).reshape(slots_n)
        grad_gates = jnp.take(back_gate, send_row, mode='fill', fill_value=0).reshape(tok_n, 1)
        g_rows = (recv_dy.astype(f32) * recv_gate[..., None]).astype(bf16)

        pos = jnp.arange(rows_loc, dtype=jnp.int32)

        def compact_of(e):
            src = pos
            for b in range(1, ep_n):
                src = src + jnp.where(pos >= starts[b, e], slot_cap - mine[b - 1, e], 0)
            src = jnp.minimum(src, rows_loc - 1)
            take = lambda a: jnp.take(a[e], src, axis=0, mode='clip')
            g = jnp.where((pos < filled[e])[:, None], take(g_rows), 0)
            x = take(x_disp)
            x_keep = lax.dynamic_slice(x, (0, me_q * w_half), (rows_loc, w_half))
            x_send = lax.dynamic_slice(x, (0, (1 - me_q) * w_half), (rows_loc, w_half))
            return take(h_gate), take(h_up), g, x_keep, x_send

        def rows_at(a, i):
            return lax.dynamic_slice(a, (i * CHUNK, 0), (CHUNK, a.shape[1]))

        def pull(packed, i):
            h1, h3, g, _, x = packed
            return tuple(lax.ppermute(rows_at(a, i), 'fsdp', swap) for a in (h1, h3, g, x))

        def grads(e, packed, i, recv, acc):
            c_pos = i * CHUNK + jnp.arange(CHUNK, dtype=jnp.int32)
            valid = jnp.concatenate([c_pos < filled[e], c_pos < filled_peer[e]])[:, None]
            h1, h3, g, x = (jnp.concatenate([rows_at(a, i), b]) for a, b in zip(packed[:4], recv))
            h3 = jnp.where(valid, h3, 0)
            d_act = jnp.einsum('rd,fd->rf', g, full_w_down[e], preferred_element_type=f32)
            gate_pre, up_pre = h1.astype(f32), h3.astype(f32)
            sig = jax.nn.sigmoid(gate_pre)
            dh1 = (d_act * up_pre * sig * (1.0 + gate_pre * (1.0 - sig))).astype(bf16)
            dh3 = (d_act * (gate_pre * sig)).astype(bf16)
            h1_half = lax.dynamic_slice(h1, (0, me_q * h_half), (2 * CHUNK, h_half)).astype(f32)
            h3_half = lax.dynamic_slice(h3, (0, me_q * h_half), (2 * CHUNK, h_half)).astype(f32)
            act = (h1_half * jax.nn.sigmoid(h1_half) * h3_half).astype(bf16)
            dx = (jnp.einsum('rf,df->rd', dh1, w_gate[e], preferred_element_type=f32) + jnp.einsum('rf,df->rd', dh3, w_up[e], preferred_element_type=f32)).astype(bf16)
            a1, a2, a3 = acc
            a1 = a1 + jnp.einsum('rd,rf->df', x, dh1, preferred_element_type=f32)
            a2 = a2 + jnp.einsum('rf,rd->fd', act, g, preferred_element_type=f32)
            a3 = a3 + jnp.einsum('rd,rf->df', x, dh3, preferred_element_type=f32)
            return dx[:CHUNK], dx[CHUNK:], (a1, a2, a3)

        def put_dx(dx_buf, i, dx_mine, dx_back):
            dx_buf = lax.dynamic_update_slice(dx_buf, dx_mine, (i * CHUNK, me_q * w_half))
            return lax.dynamic_update_slice(dx_buf, dx_back, (i * CHUNK, (1 - me_q) * w_half))

        packed = [compact_of(e) for e in range(e_loc)]
        accs, backs = [], []
        for e in range(e_loc):
            n = chunks[e]
            acc = (jnp.zeros((w_half, hid), f32), jnp.zeros((h_half, width), f32), jnp.zeros((w_half, hid), f32))
            dx_buf = jnp.zeros((rows_loc, width), bf16)
            recv = pull(packed[e], 0)

            def body(i, carry, e=e):
                recv, acc, dx_buf = carry
                nxt = pull(packed[e], i)
                dx_mine, dx_peer, acc = grads(e, packed[e], i - 1, recv, acc)
                dx_back = lax.ppermute(dx_peer, 'fsdp', swap)
                return nxt, acc, put_dx(dx_buf, i - 1, dx_mine, dx_back)

            recv, acc, dx_buf = lax.fori_loop(1, n, body, (recv, acc, dx_buf))
            dx_mine, dx_peer, acc = grads(e, packed[e], n - 1, recv, acc)
            dx_buf = put_dx(dx_buf, n - 1, dx_mine, lax.ppermute(dx_peer, 'fsdp', swap))
            accs.append(acc)
            spread = (starts[:, e][:, None] + jnp.arange(slot_cap, dtype=jnp.int32)[None, :]).reshape(-1)
            dx_rows = jnp.take(dx_buf, spread, axis=0, mode='clip').reshape(ep_n, slot_cap, width)
            backs.append(lax.all_to_all(dx_rows, 'ep', 0, 0, tiled=True).reshape(rows_loc, width))
        back_dx = jnp.concatenate(backs)
        grad_x = jnp.take(back_dx, send_row, axis=0, mode='fill', fill_value=0)
        grad_w = tuple(jnp.stack([a[k] for a in accs]) for k in range(3))
        return (grad_x, grad_gates) + grad_w

    return jax.shard_map(local_backward, mesh=mesh, in_specs=(tok_spec, tok_spec, tok_spec, tok_spec, row_spec, row_spec, row_spec, row_spec, row_spec, row_spec, row_spec), out_specs=(tok_spec, tok_spec, row_spec, row_spec, row_spec), check_vma=False)
```

```python
import functools

import jax
import jax.numpy as jnp
from jax import lax
from jax.experimental import pallas as pl
from jax.experimental.pallas import tpu as pltpu
from jax.sharding import PartitionSpec as P

CHUNK = 128
UNIT = 8
TILE = 768
F32, BF16, I32 = jnp.float32, jnp.bfloat16, jnp.int32


def dot_nt(a, b):
    return lax.dot_general(a, b, (((1,), (1,)), ((), ())), preferred_element_type=F32)


def dot_tn(a, b):
    return lax.dot_general(a, b, (((0,), (0,)), ((), ())), preferred_element_type=F32)


def seg_tiles(tab, side, s):
    first = tab[side, s - 1] if s else 0
    return first, tab[side, s]


def touched(tab, i, e):
    segs = tab.shape[1] // 2
    lo, hi = i * (CHUNK // UNIT), (i + 1) * (CHUNK // UNIT)
    one = ((tab[0, segs // 2 - 1] < hi) & (tab[0, segs - 1] > lo)) | ((tab[1, segs // 2 - 1] < hi) & (tab[1, segs - 1] > lo))
    zero = (tab[0, segs // 2 - 1] > lo) | (tab[1, segs // 2 - 1] > lo) | jnp.logical_not(one)
    return jnp.where(e == 0, zero, one)


def expert_at(tab, i, turn):
    return jnp.where(touched(tab, i, 1), turn, 1 - turn)


def pack_kernel(tab, me, step, h1, h3, g, x, dx, out, keep, sems, dx_sem):
    segs = tab.shape[1] // 2
    all_units = h1.shape[0] // UNIT
    hid, width, w_half = h1.shape[1], g.shape[1], keep.shape[1]
    mine = pl.multiple_of(me[0] * w_half, 128)
    other = pl.multiple_of((1 - me[0]) * w_half, 128)

    def copies(k):
        t = step[0] * (CHUNK // UNIT) + k
        src = t
        for s in range(segs - 1):
            first, last = seg_tiles(tab, 0, s)
            src = src + jnp.where(t >= last, all_units // segs - (last - first), 0)
        rows = pl.ds(pl.multiple_of(jnp.minimum(src, all_units - 1) * UNIT, UNIT), UNIT)
        to = pl.ds(pl.multiple_of(k * UNIT, UNIT), UNIT)
        return [
            pltpu.make_async_copy(h1.at[rows, :], out.at[to, pl.ds(0, hid)], sems.at[k, 0]),
            pltpu.make_async_copy(h3.at[rows, :], out.at[to, pl.ds(hid, hid)], sems.at[k, 1]),
            pltpu.make_async_copy(g.at[rows, :], out.at[to, pl.ds(2 * hid, width)], sems.at[k, 2]),
            pltpu.make_async_copy(x.at[rows, pl.ds(other, w_half)], out.at[to, pl.ds(2 * hid + width, w_half)], sems.at[k, 3]),
            pltpu.make_async_copy(x.at[rows, pl.ds(mine, w_half)], keep.at[to, :], sems.at[k, 4]),
        ]

    dx_copy = pltpu.make_async_copy(dx, out.at[:, pl.ds(2 * hid + width + w_half, w_half)], dx_sem)
    dx_copy.start()
    for k in range(CHUNK // UNIT):
        for c in copies(k):
            c.start()
    dx_copy.wait()
    for k in range(CHUNK // UNIT):
        for c in copies(k):
            c.wait()


def pack(tab, me, i, h1, h3, g, x, dx):
    hid, width = h1.shape[1], g.shape[1]
    anywhere = pl.BlockSpec(memory_space=pl.ANY)
    cols = 2 * hid + 2 * width
    return pl.pallas_call(
        pack_kernel,
        grid_spec=pltpu.PrefetchScalarGridSpec(
            num_scalar_prefetch=3,
            grid=(1,),
            in_specs=[anywhere] * 5,
            out_specs=[pl.BlockSpec((CHUNK, cols), lambda *_: (0, 0)), pl.BlockSpec((CHUNK, width // 2), lambda *_: (0, 0))],
            scratch_shapes=[pltpu.SemaphoreType.DMA((CHUNK // UNIT, 5)), pltpu.SemaphoreType.DMA],
        ),
        out_shape=[jax.ShapeDtypeStruct((CHUNK, cols), BF16), jax.ShapeDtypeStruct((CHUNK, width // 2), BF16)],
        compiler_params=pltpu.CompilerParams(vmem_limit_bytes=32 * 1024 * 1024, dimension_semantics=('arbitrary',)),
        cost_estimate=pl.CostEstimate(flops=4 * CHUNK * cols * 256, bytes_accessed=4 * CHUNK * cols, transcendentals=0),
    )(tab, me, i, h1, h3, g, x, dx)


def unpack_kernel(tab, me, mine, back, out, sems):
    segs = tab.shape[1] // 2
    cap, w_half = out.shape[0] // segs, mine.shape[1]
    work = []
    for s in range(segs):
        first, _ = seg_tiles(tab, 0, s)
        rows = pl.ds(pl.multiple_of(2 * CHUNK + first * UNIT, UNIT), cap)
        for k, (buf, half) in enumerate(((mine, me[0]), (back, 1 - me[0]))):
            cols = pl.ds(pl.multiple_of(half * w_half, 128), w_half)
            work.append(pltpu.make_async_copy(buf.at[rows, :], out.at[pl.ds(s * cap, cap), cols], sems.at[s, k]))
    for c in work:
        c.start()
    for c in work:
        c.wait()


def unpack(tab, me, mine, back, slots_n):
    width = 2 * mine.shape[1]
    return pl.pallas_call(
        unpack_kernel,
        grid_spec=pltpu.PrefetchScalarGridSpec(
            num_scalar_prefetch=2,
            grid=(1,),
            in_specs=[pl.BlockSpec(memory_space=pl.ANY)] * 2,
            out_specs=pl.BlockSpec((slots_n, width), lambda *_: (0, 0)),
            scratch_shapes=[pltpu.SemaphoreType.DMA((tab.shape[1] // 2, 2))],
        ),
        out_shape=jax.ShapeDtypeStruct((slots_n, width), BF16),
        compiler_params=pltpu.CompilerParams(vmem_limit_bytes=32 * 1024 * 1024, dimension_semantics=('arbitrary',)),
    )(tab, me, mine, back)


def chunk_kernel(tiles, do_dw, do_dx, tab, me, step, *refs):
    refs = list(refs)
    take = lambda n: [refs.pop(0) for _ in range(n)]
    h1_a, h3_a, g_a, x_a, h1_b, h3_b, g_b, x_b, d_b, w2_a, w2_b, w1, w3 = take(13)
    i1, i2, i3 = take(3) if do_dw else (None,) * 3
    if do_dx:
        take(2)
    o1, o2, o3 = take(3) if do_dw else (None,) * 3
    dx_b, o4, o5, sum_a, sum_b = take(5) if do_dx else (None,) * 5
    e, t = expert_at(tab, step[0], pl.program_id(0)), pl.program_id(1)
    half = tiles // 2
    segs = tab.shape[1] // 2

    if do_dx:
        @pl.when((pl.program_id(0) == 0) & (t == 0))
        def _():
            sum_a[...] = jnp.zeros_like(sum_a)
            sum_b[...] = jnp.zeros_like(sum_b)

    @pl.when(touched(tab, step[0], e))
    def _():
        w2 = jnp.where(t // half == me[0], w2_a[0], w2_b[0])
        row = step[0] * CHUNK + lax.broadcasted_iota(I32, (CHUNK, 1), 0)

        def part(side, h1_ref, h3_ref, g_ref, total):
            here = row < -CHUNK
            for s in range(segs):
                first, _ = seg_tiles(tab, side, s)
                fill = jnp.where(e == s // (segs // 2), tab[side, segs + s], 0)
                here = here | ((row >= first * UNIT) & (row < first * UNIT + fill))
            h1, h3 = h1_ref[...].astype(F32), h3_ref[...].astype(F32)
            sig = jax.nn.sigmoid(h1)
            silu = h1 * sig
            da = jnp.where(here, dot_nt(g_ref[...], w2), 0.0)
            dh1 = (da * h3 * sig * (1.0 + h1 * (1.0 - sig))).astype(BF16)
            dh3 = (da * silu).astype(BF16)
            act = jnp.where(here, silu * h3, 0.0).astype(BF16)
            if do_dx:
                total[...] += dot_nt(dh1, w1[0]) + dot_nt(dh3, w3[0])
            return dh1, dh3, act

        dh1_a, dh3_a, act_a = part(0, h1_a, h3_a, g_a, sum_a)
        dh1_b, dh3_b, act_b = part(1, h1_b, h3_b, g_b, sum_b)
        if do_dw:
            o1[0] = i1[0] + (dot_tn(x_a[...], dh1_a) + dot_tn(x_b[...], dh1_b))
            o3[0] = i3[0] + (dot_tn(x_a[...], dh3_a) + dot_tn(x_b[...], dh3_b))

            @pl.when(t // half == me[0])
            def _():
                o2[0] = i2[0] + (dot_tn(act_a, g_a[...]) + dot_tn(act_b, g_b[...]))

    if do_dx:
        @pl.when((pl.program_id(0) == 1) & (t == tiles - 1))
        def _():
            dx_b[...] = sum_b[...].astype(BF16)
            o4[...] = sum_a[...].astype(BF16)
            o5[...] = d_b[...]


def chunk_grads(tab, me, i, own, keep, got, w2, far_w2, w1, w3, acc, dx_bufs):
    rows, w_half = keep.shape
    e_loc, hid, width = w2.shape[0], 2 * w2.shape[1], w2.shape[2]
    tiles = hid // TILE
    half = tiles // 2

    def where_to(e, t, tab, step):
        e = expert_at(tab, step[0], e)
        on = touched(tab, step[0], e)
        return jnp.where(on, e, 1 - e), jnp.where(on, t, 0)

    def cols_at(first, moves):
        return lambda e, t, tab, me, step: (0, first + (where_to(e, t, tab, step)[1] if moves else 0))

    def w_col(e, t, tab, me, step):
        ee, tt = where_to(e, t, tab, step)
        return ee, 0, tt

    def w_half_row(e, t, tab, me, step):
        ee, tt = where_to(e, t, tab, step)
        return ee, jnp.clip(tt - me[0] * half, 0, half - 1), 0

    def w_far_row(e, t, tab, me, step):
        ee, tt = where_to(e, t, tab, step)
        return ee, jnp.clip(tt - (1 - me[0]) * half, 0, half - 1), 0

    shared = [pl.BlockSpec((rows, TILE), cols_at(0, True)), pl.BlockSpec((rows, TILE), cols_at(tiles, True)), pl.BlockSpec((rows, width), cols_at(2 * hid // width, False))]
    x_own = pl.BlockSpec((rows, w_half), cols_at(0, False))
    x_got = pl.BlockSpec((rows, w_half), cols_at((2 * hid + width) // w_half, False))
    dx_got = pl.BlockSpec((rows, w_half), cols_at((2 * hid + width) // w_half + 1, False))
    dx_at = lambda late: pl.BlockSpec((rows, w_half), lambda e, t, tab, me, step: (jnp.maximum(step[0] + late, 0), 0))
    anywhere = pl.BlockSpec(memory_space=pl.ANY)
    weights = [pl.BlockSpec((1, TILE, width), w_half_row), pl.BlockSpec((1, TILE, width), w_far_row), pl.BlockSpec((1, w_half, TILE), w_col), pl.BlockSpec((1, w_half, TILE), w_col)]
    grads = [pl.BlockSpec((1, w_half, TILE), w_col), pl.BlockSpec((1, TILE, width), w_half_row), pl.BlockSpec((1, w_half, TILE), w_col)]
    do_dw, do_dx = acc is not None, dx_bufs is not None
    given, in_specs, out_specs, out_shape, scratch = [], [], [], [], []
    if do_dw:
        given += acc
        in_specs += grads
        out_specs += grads
        out_shape += [jax.ShapeDtypeStruct(v.shape, F32) for v in acc]
    if do_dx:
        given += dx_bufs
        in_specs += [anywhere, anywhere]
        out_specs += [x_own, dx_at(2), dx_at(0)]
        out_shape += [jax.ShapeDtypeStruct((rows, w_half), BF16)] + [jax.ShapeDtypeStruct(v.shape, BF16) for v in dx_bufs]
        scratch = [pltpu.VMEM((rows, w_half), F32), pltpu.VMEM((rows, w_half), F32)]
    n_dw = 3 if do_dw else 0
    aliases = {16 + k: k for k in range(n_dw)}
    if do_dx:
        aliases.update({16 + n_dw: n_dw + 1, 17 + n_dw: n_dw + 2})
    out = pl.pallas_call(
        functools.partial(chunk_kernel, tiles, do_dw, do_dx),
        grid_spec=pltpu.PrefetchScalarGridSpec(
            num_scalar_prefetch=3,
            grid=(e_loc, tiles),
            in_specs=shared + [x_own] + shared + [x_got, dx_got] + weights + in_specs,
            out_specs=out_specs,
            scratch_shapes=scratch,
        ),
        out_shape=out_shape,
        input_output_aliases=aliases,
        compiler_params=pltpu.CompilerParams(vmem_limit_bytes=56 * 1024 * 1024, dimension_semantics=('arbitrary', 'arbitrary')),
        cost_estimate=pl.CostEstimate(flops=2 * rows * 7 * hid * w_half * 2, bytes_accessed=48 * 1024 * 1024, transcendentals=2 * rows * hid),
    )(tab, me, i, own, own, own, keep, got, got, got, got, got, w2, far_w2, w1, w3, *given)
    return out[n_dw] if do_dx else None, tuple(out[:3]) if do_dw else None, tuple(out[n_dw + 1:]) if do_dx else None


def solution(mesh):
    ep_n = mesh.shape['ep']
    fs_n = mesh.shape['fsdp']
    tok_spec = P(('fsdp', 'ep'), None)
    row_spec = P('ep', 'fsdp', None)
    swap = [(0, 1), (1, 0)]

    def local_backward(grad_out, expert_idx, slot_pos, gates, x_disp, h_gate, h_up, y_disp, w_gate, w_down, w_up):
        tok_n = expert_idx.shape[0]
        e_loc, rows_loc, width = x_disp.shape
        hid = h_gate.shape[2]
        w_half, h_half = width // fs_n, hid // fs_n
        slot_cap = rows_loc // ep_n
        segs = e_loc * ep_n
        slots_n = segs * slot_cap
        me_q = lax.axis_index('fsdp')


        ids, slots = expert_idx[:, 0], slot_pos[:, 0]
        hits = (ids[:, None] == jnp.arange(e_loc * ep_n, dtype=I32)[None, :]) & (slots >= 0)[:, None]
        far_counts = lax.ppermute(jnp.sum(hits.astype(F32), axis=0), 'fsdp', swap)
        far_w_down = lax.ppermute(w_down, 'fsdp', swap)
        send_row = jnp.where(slots >= 0, ((ids % e_loc) * ep_n + ids // e_loc) * slot_cap + slots, slots_n)
        src_choice = jnp.full((slots_n,), tok_n, I32).at[send_row].set(jnp.arange(tok_n, dtype=I32), mode='drop')
        send_dy = jnp.take(grad_out, src_choice, axis=0, mode='fill', fill_value=0).reshape(e_loc, ep_n, slot_cap, width)
        src_choice, send_dy = lax.optimization_barrier((src_choice, send_dy))
        recv_dy = lax.all_to_all(send_dy, 'ep', 1, 1, tiled=True).reshape(slots_n, width)
        send_gate = jnp.take(gates.reshape(-1), src_choice, mode='fill', fill_value=-1).reshape(e_loc, ep_n, slot_cap)
        far_counts = jnp.broadcast_to(far_counts.reshape(ep_n, e_loc).T[:, :, None], (e_loc, ep_n, 128 - slot_cap % 128))
        recv = lax.all_to_all(jnp.concatenate([send_gate, far_counts], axis=2), 'ep', 1, 1, tiled=True).reshape(segs, -1)
        recv_gate, far_counts = recv[:, :slot_cap], recv[:, slot_cap].astype(I32)
        acc = (jnp.zeros((e_loc, w_half, hid), F32), jnp.zeros((e_loc, h_half, width), F32), jnp.zeros((e_loc, w_half, hid), F32))
        dx_mine = jnp.zeros(((slots_n // CHUNK + 3) * CHUNK + slot_cap, w_half), BF16)
        dx_back = jnp.zeros(((slots_n // CHUNK + 3) * CHUNK + slot_cap, w_half), BF16)
        dx_wait = jnp.zeros((CHUNK, w_half), BF16)
        recv_gate, acc, dx_mine, dx_back, dx_wait = lax.optimization_barrier((recv_gate, acc, dx_mine, dx_back, dx_wait))
        dgate_rows = jnp.sum(recv_dy.astype(F32) * y_disp.reshape(slots_n, width).astype(F32), axis=1)
        back_gate = lax.all_to_all(dgate_rows.reshape(e_loc, ep_n, slot_cap), 'ep', 1, 1, tiled=True).reshape(slots_n)

        counts = jnp.sum((recv_gate >= 0).astype(I32), axis=1)
        counts = jnp.stack([counts, far_counts])
        units = jnp.cumsum((counts + UNIT - 1) // UNIT, axis=1)
        tab = jnp.concatenate([units, counts], axis=1)
        chunks = (jnp.max(units[:, segs - 1]) * UNIT + CHUNK - 1) // CHUNK
        me = me_q.astype(I32).reshape(1)
        g_rows = (recv_dy.astype(F32) * recv_gate.reshape(slots_n, 1)).astype(BF16)
        rows = (h_gate.reshape(slots_n, hid), h_up.reshape(slots_n, hid), g_rows, x_disp.reshape(slots_n, width))

        def load(i, dx):
            return pack(tab, me, jnp.asarray(i, I32).reshape(1), *rows, dx)

        def grads(i, own, keep, got, sums):
            return chunk_grads(tab, me, jnp.asarray(i, I32).reshape(1), own, keep, got, w_down, far_w_down, w_gate, w_up, *sums)

        def send(v):
            return lax.ppermute(v, 'fsdp', swap)

        dx_wait, back_gate, acc, dx_mine, dx_back = lax.optimization_barrier((dx_wait, back_gate, acc, dx_mine, dx_back))
        even = load(0, dx_wait)

        def body(k, carry):
            even, odd, got, _, sums = carry
            i = 2 * k
            got_even = send(even[0])
            dx, *sums = grads(i - 1, *odd, got, sums)
            odd = load(i + 1, dx)
            got = send(odd[0])
            dx_wait, *sums = grads(i, *even, got_even, sums)
            return load(i + 2, dx_wait), odd, got, dx_wait, tuple(sums)

        def single(k, carry):
            even, odd, got, _, sums = carry
            got_even = send(even[0])
            dx_wait, *sums = grads(chunks - 2, *odd, got, sums)
            return odd, even, got_even, dx_wait, tuple(sums)

        carry = lax.fori_loop(0, chunks // 2, body, (even, even, even[0], dx_wait, (acc, (dx_mine, dx_back))))
        _, odd, got, dx_wait, sums = lax.fori_loop(0, chunks % 2, single, carry)
        acc, bufs = sums
        dx_peer, _, (dx_mine, dx_back) = grads(chunks - 1, *odd, got, (None, bufs))
        dx_back = lax.dynamic_update_slice(dx_back, send(jnp.concatenate([dx_wait, dx_peer])), (chunks * CHUNK, 0))
        acc = grads(chunks - 1, *odd, got, (acc, None))[1]

        dx_rows = unpack(tab, me, dx_mine, dx_back, slots_n).reshape(e_loc, ep_n, slot_cap, width)
        back_dx = lax.all_to_all(dx_rows, 'ep', 1, 1, tiled=True).reshape(slots_n, width)
        grad_x = jnp.take(back_dx, send_row, axis=0, mode='fill', fill_value=0)
        grad_gates = jnp.take(back_gate, send_row, mode='fill', fill_value=0).reshape(tok_n, 1)
        return (grad_x, grad_gates) + acc

    return jax.shard_map(local_backward, mesh=mesh, in_specs=(tok_spec, tok_spec, tok_spec, tok_spec, row_spec, row_spec, row_spec, row_spec, row_spec, row_spec, row_spec), out_specs=(tok_spec, tok_spec, row_spec, row_spec, row_spec), check_vma=False)
```

```python
import functools

import jax
import jax.numpy as jnp
from jax import lax
from jax.experimental import pallas as pl
from jax.experimental.pallas import tpu as pltpu
from jax.sharding import PartitionSpec as P

CHUNK = 128
UNIT = 8
TILE = 768
F32, BF16, I32 = jnp.float32, jnp.bfloat16, jnp.int32


def dot_nt(a, b):
    return lax.dot_general(a, b, (((1,), (1,)), ((), ())), preferred_element_type=F32)


def dot_tn(a, b):
    return lax.dot_general(a, b, (((0,), (0,)), ((), ())), preferred_element_type=F32)


def seg_tiles(tab, side, s):
    first = tab[side, s - 1] if s else 0
    return first, tab[side, s]


def touched(tab, i, e):
    segs = tab.shape[1] // 2
    lo, hi = i * (CHUNK // UNIT), (i + 1) * (CHUNK // UNIT)
    one = ((tab[0, segs // 2 - 1] < hi) & (tab[0, segs - 1] > lo)) | ((tab[1, segs // 2 - 1] < hi) & (tab[1, segs - 1] > lo))
    zero = (tab[0, segs // 2 - 1] > lo) | (tab[1, segs // 2 - 1] > lo) | jnp.logical_not(one)
    return jnp.where(e == 0, zero, one) | (i < 0)


def expert_at(tab, i, turn):
    return jnp.where(touched(tab, i, 1), turn, 1 - turn)


def pack_kernel(tab, me, step, h1, h3, g, x, dx, out, keep, sems, dx_sem):
    segs = tab.shape[1] // 2
    all_units = h1.shape[0] // UNIT
    hid, width, w_half = h1.shape[1], g.shape[1], keep.shape[1]
    mine = pl.multiple_of(me[0] * w_half, 128)
    other = pl.multiple_of((1 - me[0]) * w_half, 128)

    def copies(k):
        t = step[0] * (CHUNK // UNIT) + k
        src = t
        for s in range(segs - 1):
            first, last = seg_tiles(tab, 0, s)
            src = src + jnp.where(t >= last, all_units // segs - (last - first), 0)
        rows = pl.ds(pl.multiple_of(jnp.minimum(src, all_units - 1) * UNIT, UNIT), UNIT)
        to = pl.ds(pl.multiple_of(k * UNIT, UNIT), UNIT)
        return [
            pltpu.make_async_copy(h1.at[rows, :], out.at[to, pl.ds(0, hid)], sems.at[k, 0]),
            pltpu.make_async_copy(h3.at[rows, :], out.at[to, pl.ds(hid, hid)], sems.at[k, 1]),
            pltpu.make_async_copy(g.at[rows, :], out.at[to, pl.ds(2 * hid, width)], sems.at[k, 2]),
            pltpu.make_async_copy(x.at[rows, pl.ds(other, w_half)], out.at[to, pl.ds(2 * hid + width, w_half)], sems.at[k, 3]),
            pltpu.make_async_copy(x.at[rows, pl.ds(mine, w_half)], keep.at[to, :], sems.at[k, 4]),
        ]

    dx_copy = pltpu.make_async_copy(dx, out.at[:, pl.ds(2 * hid + width + w_half, w_half)], dx_sem)
    dx_copy.start()
    for k in range(CHUNK // UNIT):
        for c in copies(k):
            c.start()
    dx_copy.wait()
    for k in range(CHUNK // UNIT):
        for c in copies(k):
            c.wait()


def pack(tab, me, i, h1, h3, g, x, dx):
    hid, width = h1.shape[1], g.shape[1]
    anywhere = pl.BlockSpec(memory_space=pl.ANY)
    cols = 2 * hid + 2 * width
    return pl.pallas_call(
        pack_kernel,
        grid_spec=pltpu.PrefetchScalarGridSpec(
            num_scalar_prefetch=3,
            grid=(1,),
            in_specs=[anywhere] * 5,
            out_specs=[pl.BlockSpec((CHUNK, cols), lambda *_: (0, 0)), pl.BlockSpec((CHUNK, width // 2), lambda *_: (0, 0))],
            scratch_shapes=[pltpu.SemaphoreType.DMA((CHUNK // UNIT, 5)), pltpu.SemaphoreType.DMA],
        ),
        out_shape=[jax.ShapeDtypeStruct((CHUNK, cols), BF16), jax.ShapeDtypeStruct((CHUNK, width // 2), BF16)],
        compiler_params=pltpu.CompilerParams(vmem_limit_bytes=32 * 1024 * 1024, dimension_semantics=('arbitrary',)),
        cost_estimate=pl.CostEstimate(flops=4 * CHUNK * cols * 256, bytes_accessed=4 * CHUNK * cols, transcendentals=0),
    )(tab, me, i, h1, h3, g, x, dx)


def unpack_kernel(tab, me, mine, back, out, sems):
    segs = tab.shape[1] // 2
    cap, w_half = out.shape[0] // segs, mine.shape[1]
    work = []
    for s in range(segs):
        first, _ = seg_tiles(tab, 0, s)
        rows = pl.ds(pl.multiple_of(2 * CHUNK + first * UNIT, UNIT), cap)
        for k, (buf, half) in enumerate(((mine, me[0]), (back, 1 - me[0]))):
            cols = pl.ds(pl.multiple_of(half * w_half, 128), w_half)
            work.append(pltpu.make_async_copy(buf.at[rows, :], out.at[pl.ds(s * cap, cap), cols], sems.at[s, k]))
    for c in work:
        c.start()
    for c in work:
        c.wait()


def unpack(tab, me, mine, back, slots_n):
    width = 2 * mine.shape[1]
    return pl.pallas_call(
        unpack_kernel,
        grid_spec=pltpu.PrefetchScalarGridSpec(
            num_scalar_prefetch=2,
            grid=(1,),
            in_specs=[pl.BlockSpec(memory_space=pl.ANY)] * 2,
            out_specs=pl.BlockSpec((slots_n, width), lambda *_: (0, 0)),
            scratch_shapes=[pltpu.SemaphoreType.DMA((tab.shape[1] // 2, 2))],
        ),
        out_shape=jax.ShapeDtypeStruct((slots_n, width), BF16),
        compiler_params=pltpu.CompilerParams(vmem_limit_bytes=32 * 1024 * 1024, dimension_semantics=('arbitrary',)),
    )(tab, me, mine, back)


def chunk_kernel(tiles, do_dw, do_dx, tab, me, step, *refs):
    refs = list(refs)
    take = lambda n: [refs.pop(0) for _ in range(n)]
    h1_a, h3_a, g_a, x_a, h1_b, h3_b, g_b, x_b, d_b, w2_a, w2_b, w1, w3 = take(13)
    i1, i2, i3 = take(3) if do_dw else (None,) * 3
    if do_dx:
        take(2)
    o1, o2, o3 = take(3) if do_dw else (None,) * 3
    dx_b, o4, o5, sum_a, sum_b = take(5) if do_dx else (None,) * 5
    e, t = expert_at(tab, step[0], pl.program_id(0)), pl.program_id(1)
    half = tiles // 2
    segs = tab.shape[1] // 2

    if do_dx:
        @pl.when((pl.program_id(0) == 0) & (t == 0))
        def _():
            sum_a[...] = jnp.zeros_like(sum_a)
            sum_b[...] = jnp.zeros_like(sum_b)

    @pl.when(touched(tab, step[0], e))
    def _():
        w2 = jnp.where(t // half == me[0], w2_a[0], w2_b[0])
        row = step[0] * CHUNK + lax.broadcasted_iota(I32, (CHUNK, 1), 0)

        def part(side, h1_ref, h3_ref, g_ref, total):
            here = row < -CHUNK
            for s in range(segs):
                first, _ = seg_tiles(tab, side, s)
                fill = jnp.where(e == s // (segs // 2), tab[side, segs + s], 0)
                here = here | ((row >= first * UNIT) & (row < first * UNIT + fill))
            h1, h3 = h1_ref[...].astype(F32), h3_ref[...].astype(F32)
            sig = jax.nn.sigmoid(h1)
            silu = h1 * sig
            da = jnp.where(here, dot_nt(g_ref[...], w2), 0.0)
            dh1 = (da * h3 * sig * (1.0 + h1 * (1.0 - sig))).astype(BF16)
            dh3 = (da * silu).astype(BF16)
            act = jnp.where(here, silu * h3, 0.0).astype(BF16)
            if do_dx:
                total[...] += dot_nt(dh1, w1[0]) + dot_nt(dh3, w3[0])
            return dh1, dh3, act

        dh1_a, dh3_a, act_a = part(0, h1_a, h3_a, g_a, sum_a)
        dh1_b, dh3_b, act_b = part(1, h1_b, h3_b, g_b, sum_b)
        if do_dw:
            o1[0] = jnp.where(step[0] < 0, 0.0, i1[0] + (dot_tn(x_a[...], dh1_a) + dot_tn(x_b[...], dh1_b)))
            o3[0] = jnp.where(step[0] < 0, 0.0, i3[0] + (dot_tn(x_a[...], dh3_a) + dot_tn(x_b[...], dh3_b)))

            @pl.when(t // half == me[0])
            def _():
                o2[0] = jnp.where(step[0] < 0, 0.0, i2[0] + (dot_tn(act_a, g_a[...]) + dot_tn(act_b, g_b[...])))

    if do_dx:
        @pl.when((pl.program_id(0) == 1) & (t == tiles - 1))
        def _():
            dx_b[...] = sum_b[...].astype(BF16)
            o4[...] = sum_a[...].astype(BF16)
            o5[...] = d_b[...]


def chunk_grads(tab, me, i, own, keep, got, w2, far_w2, w1, w3, acc, dx_bufs):
    rows, w_half = keep.shape
    e_loc, hid, width = w2.shape[0], 2 * w2.shape[1], w2.shape[2]
    tiles = hid // TILE
    half = tiles // 2

    def where_to(e, t, tab, step):
        e = expert_at(tab, step[0], e)
        on = touched(tab, step[0], e)
        return jnp.where(on, e, 1 - e), jnp.where(on, t, 0)

    def cols_at(first, moves):
        return lambda e, t, tab, me, step: (0, first + (where_to(e, t, tab, step)[1] if moves else 0))

    def w_col(e, t, tab, me, step):
        ee, tt = where_to(e, t, tab, step)
        return ee, 0, tt

    def w_half_row(e, t, tab, me, step):
        ee, tt = where_to(e, t, tab, step)
        return ee, jnp.clip(tt - me[0] * half, 0, half - 1), 0

    def w_far_row(e, t, tab, me, step):
        ee, tt = where_to(e, t, tab, step)
        return ee, jnp.clip(tt - (1 - me[0]) * half, 0, half - 1), 0

    shared = [pl.BlockSpec((rows, TILE), cols_at(0, True)), pl.BlockSpec((rows, TILE), cols_at(tiles, True)), pl.BlockSpec((rows, width), cols_at(2 * hid // width, False))]
    x_own = pl.BlockSpec((rows, w_half), cols_at(0, False))
    x_got = pl.BlockSpec((rows, w_half), cols_at((2 * hid + width) // w_half, False))
    dx_got = pl.BlockSpec((rows, w_half), cols_at((2 * hid + width) // w_half + 1, False))
    dx_at = lambda late: pl.BlockSpec((rows, w_half), lambda e, t, tab, me, step: (jnp.maximum(step[0] + late, 0), 0))
    anywhere = pl.BlockSpec(memory_space=pl.ANY)
    weights = [pl.BlockSpec((1, TILE, width), w_half_row), pl.BlockSpec((1, TILE, width), w_far_row), pl.BlockSpec((1, w_half, TILE), w_col), pl.BlockSpec((1, w_half, TILE), w_col)]
    grads = [pl.BlockSpec((1, w_half, TILE), w_col), pl.BlockSpec((1, TILE, width), w_half_row), pl.BlockSpec((1, w_half, TILE), w_col)]
    do_dw, do_dx = acc is not None, dx_bufs is not None
    given, in_specs, out_specs, out_shape, scratch = [], [], [], [], []
    if do_dw:
        given += acc
        in_specs += grads
        out_specs += grads
        out_shape += [jax.ShapeDtypeStruct(v.shape, F32) for v in acc]
    if do_dx:
        given += dx_bufs
        in_specs += [anywhere, anywhere]
        out_specs += [x_own, dx_at(2), dx_at(0)]
        out_shape += [jax.ShapeDtypeStruct((rows, w_half), BF16)] + [jax.ShapeDtypeStruct(v.shape, BF16) for v in dx_bufs]
        scratch = [pltpu.VMEM((rows, w_half), F32), pltpu.VMEM((rows, w_half), F32)]
    n_dw = 3 if do_dw else 0
    aliases = {16 + k: k for k in range(n_dw)}
    if do_dx:
        aliases.update({16 + n_dw: n_dw + 1, 17 + n_dw: n_dw + 2})
    out = pl.pallas_call(
        functools.partial(chunk_kernel, tiles, do_dw, do_dx),
        grid_spec=pltpu.PrefetchScalarGridSpec(
            num_scalar_prefetch=3,
            grid=(e_loc, tiles),
            in_specs=shared + [x_own] + shared + [x_got, dx_got] + weights + in_specs,
            out_specs=out_specs,
            scratch_shapes=scratch,
        ),
        out_shape=out_shape,
        input_output_aliases=aliases,
        compiler_params=pltpu.CompilerParams(vmem_limit_bytes=56 * 1024 * 1024, dimension_semantics=('arbitrary', 'arbitrary')),
        cost_estimate=pl.CostEstimate(flops=2 * rows * 7 * hid * w_half * 2, bytes_accessed=48 * 1024 * 1024, transcendentals=2 * rows * hid),
    )(tab, me, i, own, own, own, keep, got, got, got, got, got, w2, far_w2, w1, w3, *given)
    return out[n_dw] if do_dx else None, tuple(out[:3]) if do_dw else None, tuple(out[n_dw + 1:]) if do_dx else None


def room(shapes):
    return tuple(pl.pallas_call(lambda *refs: None, out_shape=[jax.ShapeDtypeStruct(v, F32) for v in shapes], out_specs=[pl.BlockSpec(memory_space=pl.ANY)] * len(shapes))())


def solution(mesh):
    ep_n = mesh.shape['ep']
    fs_n = mesh.shape['fsdp']
    tok_spec = P(('fsdp', 'ep'), None)
    row_spec = P('ep', 'fsdp', None)
    swap = [(0, 1), (1, 0)]

    def local_backward(grad_out, expert_idx, slot_pos, gates, x_disp, h_gate, h_up, y_disp, w_gate, w_down, w_up):
        tok_n = expert_idx.shape[0]
        e_loc, rows_loc, width = x_disp.shape
        hid = h_gate.shape[2]
        w_half, h_half = width // fs_n, hid // fs_n
        slot_cap = rows_loc // ep_n
        segs = e_loc * ep_n
        slots_n = segs * slot_cap
        me_q = lax.axis_index('fsdp')


        ids, slots = expert_idx[:, 0], slot_pos[:, 0]
        hits = (ids[:, None] == jnp.arange(e_loc * ep_n, dtype=I32)[None, :]) & (slots >= 0)[:, None]
        far_counts = lax.ppermute(jnp.sum(hits.astype(F32), axis=0), 'fsdp', swap)
        far_w_down = lax.ppermute(w_down, 'fsdp', swap)
        send_row = jnp.where(slots >= 0, ((ids % e_loc) * ep_n + ids // e_loc) * slot_cap + slots, slots_n)
        src_choice = jnp.full((slots_n,), tok_n, I32).at[send_row].set(jnp.arange(tok_n, dtype=I32), mode='drop')
        send_dy = jnp.take(grad_out, src_choice, axis=0, mode='fill', fill_value=0).reshape(e_loc, ep_n, slot_cap, width)
        src_choice, send_dy = lax.optimization_barrier((src_choice, send_dy))
        recv_dy = lax.all_to_all(send_dy, 'ep', 1, 1, tiled=True).reshape(slots_n, width)
        send_gate = jnp.take(gates.reshape(-1), src_choice, mode='fill', fill_value=-1).reshape(e_loc, ep_n, slot_cap)
        far_counts = jnp.broadcast_to(far_counts.reshape(ep_n, e_loc).T[:, :, None], (e_loc, ep_n, 128 - slot_cap % 128))
        recv = lax.all_to_all(jnp.concatenate([send_gate, far_counts], axis=2), 'ep', 1, 1, tiled=True).reshape(segs, -1)
        recv_gate, far_counts = recv[:, :slot_cap], recv[:, slot_cap].astype(I32)
        acc = room([(e_loc, w_half, hid), (e_loc, h_half, width), (e_loc, w_half, hid)])
        dx_mine = jnp.zeros(((slots_n // CHUNK + 3) * CHUNK + slot_cap, w_half), BF16)
        dx_back = jnp.zeros(((slots_n // CHUNK + 3) * CHUNK + slot_cap, w_half), BF16)
        dx_wait = jnp.zeros((CHUNK, w_half), BF16)
        recv_gate, acc, dx_mine, dx_back, dx_wait = lax.optimization_barrier((recv_gate, acc, dx_mine, dx_back, dx_wait))
        dgate_rows = jnp.sum(recv_dy.astype(F32) * y_disp.reshape(slots_n, width).astype(F32), axis=1)
        back_gate = lax.all_to_all(dgate_rows.reshape(e_loc, ep_n, slot_cap), 'ep', 1, 1, tiled=True).reshape(slots_n)

        counts = jnp.sum((recv_gate >= 0).astype(I32), axis=1)
        counts = jnp.stack([counts, far_counts])
        units = jnp.cumsum((counts + UNIT - 1) // UNIT, axis=1)
        tab = jnp.concatenate([units, counts], axis=1)
        chunks = (jnp.max(units[:, segs - 1]) * UNIT + CHUNK - 1) // CHUNK
        me = me_q.astype(I32).reshape(1)
        g_rows = (recv_dy.astype(F32) * recv_gate.reshape(slots_n, 1)).astype(BF16)
        rows = (h_gate.reshape(slots_n, hid), h_up.reshape(slots_n, hid), g_rows, x_disp.reshape(slots_n, width))

        def load(i, dx):
            return pack(tab, me, jnp.asarray(i, I32).reshape(1), *rows, dx)

        def grads(i, own, keep, got, sums):
            return chunk_grads(tab, me, jnp.asarray(i, I32).reshape(1), own, keep, got, w_down, far_w_down, w_gate, w_up, *sums)

        def send(v):
            return lax.ppermute(v, 'fsdp', swap)

        dx_wait, back_gate, acc, dx_mine, dx_back = lax.optimization_barrier((dx_wait, back_gate, acc, dx_mine, dx_back))
        even = load(0, dx_wait)

        def body(k, carry):
            even, odd, got, _, sums = carry
            i = 2 * k
            got_even = send(even[0])
            dx, *sums = grads(i - 1, *odd, got, sums)
            odd = load(i + 1, dx)
            got = send(odd[0])
            dx_wait, *sums = grads(i, *even, got_even, sums)
            return load(i + 2, dx_wait), odd, got, dx_wait, tuple(sums)

        def single(k, carry):
            even, odd, got, _, sums = carry
            got_even = send(even[0])
            dx_wait, *sums = grads(chunks - 2, *odd, got, sums)
            return odd, even, got_even, dx_wait, tuple(sums)

        carry = lax.fori_loop(0, chunks // 2, body, (even, even, even[0], dx_wait, (acc, (dx_mine, dx_back))))
        _, odd, got, dx_wait, sums = lax.fori_loop(0, chunks % 2, single, carry)
        acc, bufs = sums
        dx_peer, _, (dx_mine, dx_back) = grads(chunks - 1, *odd, got, (None, bufs))
        dx_back = lax.dynamic_update_slice(dx_back, send(jnp.concatenate([dx_wait, dx_peer])), (chunks * CHUNK, 0))
        acc = grads(chunks - 1, *odd, got, (acc, None))[1]

        dx_rows = unpack(tab, me, dx_mine, dx_back, slots_n).reshape(e_loc, ep_n, slot_cap, width)
        back_dx = lax.all_to_all(dx_rows, 'ep', 1, 1, tiled=True).reshape(slots_n, width)
        grad_x = jnp.take(back_dx, send_row, axis=0, mode='fill', fill_value=0)
        grad_gates = jnp.take(back_gate, send_row, mode='fill', fill_value=0).reshape(tok_n, 1)
        return (grad_x, grad_gates) + acc

    return jax.shard_map(local_backward, mesh=mesh, in_specs=(tok_spec, tok_spec, tok_spec, tok_spec, row_spec, row_spec, row_spec, row_spec, row_spec, row_spec, row_spec), out_specs=(tok_spec, tok_spec, row_spec, row_spec, row_spec), check_vma=False)
```
